256 devices in a mesh: expert: 64 (over z, y, core), tensor: 4 (over x).
Axes of the slice: x: 4, y: 4, z: 8, core: 2. Of those that a mesh axis runs over, the one named last changes fastest.
Arguments:
- tokens: bfloat16 [8192, 2880], P(('expert', 'tensor')), may hold values from -6 to 6
- cotangent: bfloat16 [8192, 2880], P(('expert', 'tensor')), may hold values from -6 to 6
- routes: int32 [8192, 4], P(('expert', 'tensor')), may hold values from 0 to 63, all different within a row; in each aligned block of 32 rows (0 to 31, 32 to 63, ...) at most 3 rows name the same one
- combine: float32 [8192, 4], P(('expert', 'tensor')), may hold values from 0.1 to 1
- w_gate: bfloat16 [64, 2880, 1440], P('expert', None, 'tensor'), may hold values from -0.109375 to 0.109375
- w_up: bfloat16 [64, 2880, 1440], P('expert', None, 'tensor'), may hold values from -0.109375 to 0.109375
- w_down: bfloat16 [64, 1440, 2880], P('expert', 'tensor'), may hold values from -0.15625 to 0.15625
Outputs:
- token_grad: bfloat16 [8192, 2880], P(('expert', 'tensor'))
- gate_grad: bfloat16 [64, 2880, 1440], P('expert', None, 'tensor')
- up_grad: bfloat16 [64, 2880, 1440], P('expert', None, 'tensor')
- down_grad: bfloat16 [64, 1440, 2880], P('expert', 'tensor')
The draws below stay inside these ranges and needn't reach their ends.
Inputs may be any that keep to these rules, and one draw needn't show every extreme that they name: `routes`: each row names 4 different experts. Among the rows of one device no expert is named more than 3 times, and in every draw some expert is named exactly 3 times by the rows of some device.
All inputs are finite; a program needn't handle non-finite values.
Results may differ from the reference program's by a relative error of at most 0.0065.
Values may be sent and summed in bfloat16 or wider, within the bound.
No kernel may reach another device: no remote copies, remote signals or barrier semaphores. Data moves between devices by JAX's collectives and lax.ppermute only.
A program may use at most 128 MiB of HBM per device.

```python
import math
import jax
import jax.numpy as jnp
import numpy as np
from jax import lax

D = 2880
H = 1440
TOP = 4
TOK_DEV = 32
EXPERTS = 64
CAP = 3
TOKENS = 8192
N_EXPERT = 64
N_TENSOR = 4


def levels(stream_key, shape, shards, smallest, top_value):
    level, own = 1.0, jax.random.fold_in(stream_key, 6)
    for position, shards_of in shards:
        steps = jnp.exp(jax.random.uniform(jax.random.fold_in(own, position), (shards_of,), jnp.float32, smallest / len(shards), top_value / len(shards)))
        level = level * jnp.repeat(steps, shape[position] // shards_of).reshape([-1 if axis == position else 1 for axis in range(len(shape))])
    return level


def routed_block(stream_key, own, number, rows, count, top, most, lean):
    sequence = jax.random.permutation(stream_key, count)
    packed, common = load_shares(count, rows * top, most, lean, True), load_shares(count, rows * top, most, lean, False)
    places = jnp.arange(count)

    def named(sizes, turn):
        used = int((sizes > 0).sum())
        fixed = max(1, used // 4)
        moved = fixed + (places - fixed + turn * (used - fixed)) % max(1, count - fixed)
        return jnp.zeros((count,), jnp.int32).at[sequence[jnp.where(places < fixed, places, moved)]].set(jnp.asarray(sizes, jnp.int32))

    sizes = jnp.where(number % 4 == 0, named(packed, number // 4), named(common, number - number // 4 - 1))
    mixed = jax.random.permutation(jax.random.fold_in(own, 3), count)
    giver, sink = mixed[0:count // 2 * 2:2], mixed[1:count // 2 * 2:2]
    slack = jnp.minimum(sizes[giver] - 1, most - sizes[sink]) // 2
    slack = jnp.where((giver == sequence[0]) | (sink == sequence[0]) | (sizes[sink] == 0), 0, jnp.maximum(slack, 0))
    moved = jax.random.randint(jax.random.fold_in(own, 4), (count // 2,), 0, 1 << 20) % (slack + 1)
    sizes = sizes.at[giver].add(-moved).at[sink].add(moved)
    items = jnp.searchsorted(jnp.cumsum(sizes), jnp.arange(rows * top), side="right").astype(jnp.int32)
    grid = items.reshape(top, rows).T
    grid = grid[jax.random.permutation(jax.random.fold_in(own, 1), rows)]
    turn = jax.random.randint(jax.random.fold_in(own, 2), (rows, 1), 0, top)
    return jnp.take_along_axis(grid, (jnp.arange(top)[None, :] + turn) % top, axis=1)


def load_shares(amount, total, most, lean, full):
    weights = [(1 << 20) // math.isqrt(standing ** lean) + 1 for standing in range(1, amount + 1)]
    largest = most if full else min(most, max(-(-total // amount), total * weights[0] // sum(weights)))
    least = 1 if total - largest >= amount - 1 else 0
    given, spare = [largest] + [least] * (amount - 1), total - largest - least * (amount - 1)
    while spare > 0:
        free = [i for i in range(1, amount) if given[i] < largest] or [i for i in range(1, amount) if given[i] < most]
        mass, remaining = sum([weights[i] for i in free]), spare
        for i in free:
            more = min(most - given[i], max(1, remaining * weights[i] // mass), spare)
            given[i] = given[i] + more
            spare = spare - more
    return np.array(given)


def centred(own_key, shape, deviation, bound, cuts=(), kind=jnp.bfloat16):
    factor_of = levels(own_key, shape, cuts, -0.22, 0.18) if cuts else 1.0
    array = jax.random.normal(own_key, shape, jnp.float32) * deviation * factor_of
    return jnp.minimum(jnp.maximum(array, -bound), bound).astype(kind)


def setup_inputs(seed: int = 0) -> dict:
    key_of = jax.random.split(jax.random.key(seed), 8)
    tokens = centred(key_of[0], (TOKENS, D), 1.0, 6.0, ((0, 256),))
    cotangent = centred(key_of[1], (TOKENS, D), 1.0, 6.0, ((0, 256),))
    routes_keys = jax.random.split(jax.random.fold_in(key_of[2], 1), TOKENS // TOK_DEV)
    routes_turns = jax.random.permutation(jax.random.fold_in(key_of[2], 3), TOKENS // TOK_DEV)
    routes = jax.vmap(lambda own, number: routed_block(jax.random.fold_in(key_of[2], 2), own, number, TOK_DEV, EXPERTS, TOP, CAP, 2))(routes_keys, routes_turns).reshape((TOKENS, TOP))
    combine = jnp.clip(jnp.exp(math.log(1.0) - 2.3025851 * jax.random.uniform(key_of[3], (TOKENS, TOP), jnp.float32) ** levels(key_of[3], (TOKENS, TOP), ((0, 256),), -0.2, 0.2)), 0.1, 1.0)
    w_gate = centred(key_of[4], (EXPERTS, D, H), D ** -0.5, 0.109375, ((0, 64), (2, 4)))
    w_up = centred(key_of[5], (EXPERTS, D, H), D ** -0.5, 0.109375, ((0, 64), (2, 4)))
    w_down = centred(key_of[6], (EXPERTS, H, D), H ** -0.5, 0.15625, ((0, 64), (1, 4)))
    return {"tokens": tokens, "cotangent": cotangent, "routes": routes, "combine": combine, "w_gate": w_gate, "w_up": w_up, "w_down": w_down}


def route_slots(flat, experts, cap):
    onehot = (flat[:, None] == jnp.arange(experts, dtype=jnp.int32)[None, :]).astype(jnp.int32)
    before = jnp.cumsum(onehot, axis=0) - onehot
    place = jnp.sum(before * onehot, axis=1)
    return (flat * cap + place).astype(jnp.int32)


def slot_sources(slot, count):
    target = jnp.arange(count, dtype=jnp.int32)
    match = slot[None, :] == target[:, None]
    valid = jnp.any(match, axis=1)
    order = jnp.arange(slot.shape[0], dtype=jnp.int32)
    source = jnp.sum(jnp.where(match, order[None, :], 0), axis=1).astype(jnp.int32)
    return source, valid


def reference(tokens, cotangent, routes, combine, w_gate, w_up, w_down):
    devices = N_EXPERT * N_TENSOR
    per_dev = TOK_DEV * TOP
    flat = routes.reshape(devices, per_dev).astype(jnp.int32)
    slots = jax.vmap(lambda f: route_slots(f, EXPERTS, CAP))(flat)
    source, valid = jax.vmap(lambda s: slot_sources(s, EXPERTS * CAP))(slots)
    offset = jnp.arange(devices, dtype=jnp.int32)[:, None] * per_dev
    route_index = (source + offset).astype(jnp.int32)
    route_index = route_index.reshape(devices, EXPERTS, CAP).transpose(1, 0, 2).reshape(EXPERTS, devices * CAP)
    valid = valid.reshape(devices, EXPERTS, CAP).transpose(1, 0, 2).reshape(EXPERTS, devices * CAP)
    weights_flat = combine.reshape(-1).astype(jnp.float32)

    def expert_step(items):
        e_gate, e_up, e_down, ridx, live = items
        token = (ridx // TOP).astype(jnp.int32)
        xs = jnp.where(live[:, None], tokens[token], 0).astype(tokens.dtype)
        scaled = weights_flat[ridx][:, None] * cotangent[token].astype(jnp.float32)
        dys = jnp.where(live[:, None], scaled, 0.0).astype(jnp.bfloat16)
        gate = jnp.dot(xs, e_gate, preferred_element_type=jnp.float32)
        upper = jnp.dot(xs, e_up, preferred_element_type=jnp.float32)
        sigma = jax.nn.sigmoid(gate)
        act = (gate * sigma * upper).astype(jnp.bfloat16)
        d_act = jnp.dot(dys, e_down.T, preferred_element_type=jnp.float32)
        d_down = jnp.dot(act.T, dys, preferred_element_type=jnp.float32).astype(jnp.bfloat16)
        d_upper = (d_act * gate * sigma).astype(jnp.bfloat16)
        d_gate = (d_act * upper * sigma * (1.0 + gate * (1.0 - sigma))).astype(jnp.bfloat16)
        g_grad = jnp.dot(xs.T, d_gate, preferred_element_type=jnp.float32).astype(jnp.bfloat16)
        u_grad = jnp.dot(xs.T, d_upper, preferred_element_type=jnp.float32).astype(jnp.bfloat16)
        rows = jnp.dot(d_gate, e_gate.T, preferred_element_type=jnp.float32)
        rows = rows + jnp.dot(d_upper, e_up.T, preferred_element_type=jnp.float32)
        return rows.astype(jnp.bfloat16), g_grad, u_grad, d_down

    dxs, gate_grad, up_grad, down_grad = lax.map(expert_step, (w_gate, w_up, w_down, route_index, valid))
    expert_of = flat
    place = slots - expert_of * CAP
    dev_index = jnp.arange(devices, dtype=jnp.int32)[:, None]
    row_index = (expert_of * (devices * CAP) + dev_index * CAP + place).astype(jnp.int32).reshape(-1)
    picked = dxs.reshape(EXPERTS * devices * CAP, D)[row_index].astype(jnp.float32)
    token_grad = jnp.sum(picked.reshape(TOKENS, TOP, D), axis=1).astype(jnp.bfloat16)
    return token_grad, gate_grad, up_grad, down_grad
```

```python
import jax
import jax.numpy as jnp
from jax import lax
from jax.experimental import pallas as pl
from jax.experimental.pallas import tpu as pltpu
from jax.sharding import Mesh, PartitionSpec as P

CAP = 3
TOP = 4
BF = jnp.bfloat16
F32 = jnp.float32
ZOFF = (0, 1, 7, 2, 6, 3, 5, 4)
YOFF = ((0, 0), (0, 1), (1, 0), (3, 0), (1, 1), (3, 1), (2, 0), (2, 1))
STEP = 512


def shift(v, axis, n, s):
    return lax.ppermute(v, axis, [(i, (i + s) % n) for i in range(n)])


def plane_shift(v, dy, dc):
    pairs = [
        (y * 2 + c, ((y + dy) % 4) * 2 + (c ^ dc)) for y in range(4) for c in range(2)
    ]
    return lax.ppermute(v, ("y", "core"), pairs)


def plane_gather(v):
    return [v] + [plane_shift(v, *YOFF[b]) for b in range(1, 8)]


def z_exchange(blocks, sign):
    return [blocks[0]] + [
        shift(blocks[k], "z", 8, sign * ZOFF[k]) for k in range(1, 8)
    ]


def dot(a, b, ca, cb):
    return lax.dot_general(
        a, b, (((ca,), (cb,)), ((), ())), preferred_element_type=F32
    )


def call(body, name, outs, args, flops):
    size = sum(a.size * a.dtype.itemsize for a in args)
    size += sum(o.size * o.dtype.itemsize for o in outs)
    return pl.pallas_call(
        body,
        out_shape=outs,
        name=name,
        compiler_params=pltpu.CompilerParams(vmem_limit_bytes=40 * 2**20),
        cost_estimate=pl.CostEstimate(flops=flops, bytes_accessed=size, transcendentals=0),
    )(*args)


def spans(width):
    return [(s, min(s + STEP, width)) for s in range(0, width, STEP)]


def pick_rows(picks, blocks, outs):
    width = outs[0].shape[1]
    for lo, hi in spans(width):
        rows = jnp.concatenate([b[:, lo:hi] for b in blocks], axis=0)
        got = sum(dot(p, rows, 0, 0) for p in picks)
        for k in range(8):
            outs[k][:, lo:hi] = got[k * 24 : k * 24 + 24].astype(BF)


def select_x_body(want_ref, block_ref, *refs):
    blocks, outs, picks = refs[:8], refs[8:16], refs[16:20]
    want = want_ref[...]
    home = block_ref[...]
    width = outs[0].shape[1]
    for b in range(8):
        info = blocks[b][:, 2816:2944].astype(F32)
        total = [jnp.zeros((32, 192), F32) for _ in range(4)]
        for i in range(TOP):
            hit = (info[:, 64 + i : 65 + i] == want) & (home == float(b))
            total[0] = total[0] + jnp.where(hit, 1.0, 0.0)
            for j in range(1, 4):
                c = 64 + TOP * j + i
                total[j] = total[j] + jnp.where(hit, info[:, c : c + 1], 0.0)
        for j in range(4):
            picks[j][b * 32 : b * 32 + 32, :] = total[j].astype(BF)
    pick_rows([picks[0][...]], blocks, outs)


def select_x(want, home, blocks, width):
    outs = [jax.ShapeDtypeStruct((24, width), BF)] * 8
    outs = outs + [jax.ShapeDtypeStruct((256, 192), BF)] * 4
    got = call(select_x_body, "select_x", outs, [want, home] + blocks, 2 * 192 * 256 * width)
    return got[:8], got[8], got[9:]


def select_dy_body(*refs):
    pick_rows([p[...] for p in refs[:3]], refs[3:11], refs[11:])


def select_dy(parts, blocks, width):
    outs = [jax.ShapeDtypeStruct((24, width), BF)] * 8
    return call(select_dy_body, "select_dy", outs, list(parts) + blocks, 6 * 192 * 256 * width)


def join_body(*refs):
    for lo, hi in spans(refs[8].shape[1]):
        rows = [r[:, lo:hi].astype(F32) for r in refs[:8]]
        refs[8][:, lo:hi] = jnp.concatenate(rows, axis=0).astype(BF)


def join(blocks):
    out = [jax.ShapeDtypeStruct((192, blocks[0].shape[1]), BF)]
    return call(join_body, "join", out, blocks, 1000000)[0]


def finish_body(own, left, right, *outs):
    for lo, hi in spans(own.shape[1]):
        s = own[:, lo:hi] + left[:, lo:hi].astype(F32) + right[:, lo:hi].astype(F32)
        for k in range(8):
            outs[k][:, lo:hi] = s[k * 24 : k * 24 + 24].astype(BF)


def finish(own, left, right):
    outs = [jax.ShapeDtypeStruct((24, own.shape[1]), BF)] * 8
    return call(finish_body, "finish", outs, [own, left, right], 1000000)


def spread_body(pick, *refs):
    blocks, outs = refs[:8], refs[8:]
    p = pick[...]
    for lo, hi in spans(blocks[0].shape[1]):
        rows = jnp.concatenate([r[:, lo:hi].astype(F32) for r in blocks], axis=0)
        got = dot(p, rows.astype(BF), 1, 0)
        for b in range(8):
            outs[b][:, lo:hi] = got[b * 32 : b * 32 + 32].astype(outs[b].dtype)


def spread(pick, blocks):
    width = blocks[0].shape[1]
    outs = [jax.ShapeDtypeStruct((32, width), F32 if b == 0 else BF) for b in range(8)]
    return call(spread_body, "spread", outs, [pick] + blocks, 2 * 192 * 256 * width)


def route_slots(flat, experts, cap):
    onehot = (flat[:, None] == jnp.arange(experts, dtype=jnp.int32)[None, :]).astype(BF)
    earlier = jnp.tril(jnp.ones((flat.shape[0],) * 2, BF), -1)
    place = jnp.sum(dot(earlier, onehot, 1, 0) * onehot.astype(F32), axis=1)
    return flat.astype(F32) * cap + place


def pieces(c):
    hi = lax.reduce_precision(c, 8, 7)
    rest = c - hi
    mid = lax.reduce_precision(rest, 8, 7)
    return [hi.astype(BF), mid.astype(BF), (rest - mid).astype(BF)]


def on_device(tokens, cotangent, routes, combine, w_gate, w_up, w_down):
    tok, width = tokens.shape
    slot = route_slots(routes.reshape(-1), 64, CAP).reshape(tok, TOP)
    info = jnp.concatenate([slot.astype(BF)] + pieces(combine), axis=1)
    info = jnp.pad(info, ((0, 0), (0, 64 - info.shape[1])))
    packed = jnp.concatenate([tokens, info], axis=1)

    z = lax.axis_index("z")
    mine = lax.axis_index("y") * 2 + lax.axis_index("core")
    row = jnp.arange(192, dtype=jnp.int32)
    k = row // 24
    off = jnp.where(k == 7, 4, jnp.where(k % 2 == 1, (k + 1) // 2, (8 - k // 2) % 8))
    want = ((((z + off) % 8) * 8 + mine) * CAP + row % CAP).astype(F32)[None]
    home = ((row // CAP) % 8).astype(F32)[None]

    send_x, pick, parts = select_x(want, home, plane_gather(packed), width)
    recv_x = join(z_exchange(send_x, 1))
    left_x = shift(recv_x, "x", 4, 1)
    right_x = shift(recv_x, "x", 4, -1)
    h = recv_x.shape[0] // 2

    cotangent, _ = lax.optimization_barrier((cotangent, send_x[0]))
    plane_dy = plane_gather(cotangent)
    plane_dy, _ = lax.optimization_barrier((plane_dy, recv_x))
    recv_dy = join(z_exchange(select_dy(parts, plane_dy, width), 1))
    far_x = [shift(left_x[:h], "x", 4, 1), shift(right_x[h:], "x", 4, -1)]
    left_dy = shift(recv_dy, "x", 4, 1)
    right_dy = shift(recv_dy, "x", 4, -1)
    far_dy = [shift(left_dy[:h], "x", 4, 1), shift(right_dy[h:], "x", 4, -1)]

    gate_w = w_gate[0]
    up_w = w_up[0]
    down_w = w_down[0]

    acts, d_gates, d_uppers = [], [], []
    xs_blocks = [recv_x, left_x, right_x] + far_x
    dy_blocks = [recv_dy, left_dy, right_dy] + far_dy
    for xb, db in zip(xs_blocks, dy_blocks):
        gate = dot(xb, gate_w, 1, 0)
        upper = dot(xb, up_w, 1, 0)
        sigma = jax.nn.sigmoid(gate)
        acts.append((gate * sigma * upper).astype(BF))
        d_act = dot(db, down_w, 1, 1)
        d_uppers.append((d_act * gate * sigma).astype(BF))
        d_gates.append((d_act * upper * sigma * (1.0 + gate * (1.0 - sigma))).astype(BF))

    def rows(i):
        return dot(d_gates[i], gate_w, 1, 1) + dot(d_uppers[i], up_w, 1, 1)

    a = shift(rows(3).astype(BF), "x", 4, 1)
    b = shift(rows(4).astype(BF), "x", 4, -1)
    nxt = rows(2) + jnp.pad(a, ((0, h), (0, 0))).astype(F32)
    prev = rows(1) + jnp.pad(b, ((h, 0), (0, 0))).astype(F32)
    u = shift(nxt.astype(BF), "x", 4, 1)
    w = shift(prev.astype(BF), "x", 4, -1)
    back = z_exchange(finish(rows(0), u, w), -1)
    part = spread(pick, back)
    got = [plane_shift(part[b], -YOFF[b][0], YOFF[b][1]) for b in range(1, 8)]
    token_grad = sum([g.astype(F32) for g in got], part[0]).astype(BF)

    xs = jnp.concatenate(xs_blocks, axis=0)
    dys = jnp.concatenate(dy_blocks, axis=0)
    down_grad = dot(jnp.concatenate(acts, axis=0), dys, 0, 0).astype(BF)
    gate_grad = dot(xs, jnp.concatenate(d_gates, axis=0), 0, 0).astype(BF)
    up_grad = dot(xs, jnp.concatenate(d_uppers, axis=0), 0, 0).astype(BF)
    return (token_grad, gate_grad[None], up_grad[None], down_grad[None])


def solution(mesh):
    fine = Mesh(mesh.devices.reshape(8, 4, 2, 4), ("z", "y", "core", "x"))
    rows = P(("z", "y", "core", "x"), None)
    cols = P(("z", "y", "core"), None, "x")
    down = P(("z", "y", "core"), "x", None)
    return jax.shard_map(
        on_device,
        mesh=fine,
        in_specs=(rows, rows, rows, rows, cols, cols, down),
        out_specs=(rows, cols, cols, down),
        check_vma=False,
    )
```
